32 devices in a mesh: dp: 32 (over z, y, x, core), tensor: 1.
Axes of the slice: x: 2, y: 2, z: 4, core: 2. Of those that a mesh axis runs over, the one named last changes fastest.
Arguments:
- grad_codes: bfloat16 [4, 32, 32, 18432], P(None, 'dp', None, 'tensor'), may hold values from -448 to 448
- exponents: int32 [4, 32, 16], P(None, 'dp'), may hold values from 7 to 10
- accumulated: bfloat16 [32, 18432], P('dp', 'tensor'), may hold values from -12 to 12
- arrival: int32 [32], replicated, may hold values from 0 to 31, each once
- bucket_of_row: int32 [32], replicated, may hold values from 0 to 15, never falling along the last dimension, each value on 1 to 4 neighbouring positions
Outputs:
- unit_codes: bfloat16 [4, 32, 18432], P(None, 'dp', 'tensor')
- bucket_peaks: float32 [4, 16], replicated
- compensated: float32 [32, 18432], P('dp', 'tensor')
The draws below stay inside these ranges and needn't reach their ends.
Inputs may be any that keep to these rules, and one draw needn't show every extreme that they name: `arrival`: each weight row appears in exactly one slot. `bucket_of_row`: bucket numbers never fall along the rows; each bucket holds 1 to 4 consecutive rows and one holds exactly 4.
All inputs are finite; a program needn't handle non-finite values.
Results may differ from the reference program's by a relative error of at most 0.001.
Values sent between devices are 32-bit elements; how exact they have to be, the bound alone decides.
A program may use at most 64 MiB of HBM per device.

```python
import math
import jax
import jax.numpy as jnp
import numpy as np
from jax import lax

FF = 18432
STEPS = 4
NB = 16
ROWS = 32
REPLICAS = 32
BMOST = 4


def plant(array, rng, least, high):
    longest = array.shape.index(max(array.shape))
    spots = []
    for shift in (0, 1):
        where = [jax.random.randint(jax.random.fold_in(rng, axis), (), 0, length) for axis, length in enumerate(array.shape)]
        where[longest] = (where[longest] + shift) % array.shape[longest]
        spots.append(tuple(where))
    return array.at[spots[0]].set(least).at[spots[1]].set(high)


def raised(drawn, stream_key, source, target, blocks, factor):
    def block_of(axis_at):
        return (jnp.arange(drawn.shape[axis_at]) // (drawn.shape[axis_at] // blocks)).reshape((-1,) + (1,) * (drawn.ndim - 1 - axis_at))

    first = jax.random.permutation(stream_key, blocks)[block_of(target)]
    second = (block_of(target) + blocks // 2) % blocks
    return jnp.where((block_of(source) == first) | (block_of(source) == second), factor * drawn, drawn)


def levels(stream_key, extent, shards, low, high):
    def one(position, shards_of):
        draws = jax.random.uniform(jax.random.fold_in(jax.random.fold_in(stream_key, 6), position), (shards_of,), jnp.float32, low / len(shards), high / len(shards))
        return jnp.repeat(jnp.exp(draws), extent[position] // shards_of).reshape((-1,) + (1,) * (len(extent) - position - 1))

    factor_of = one(*shards[0])
    for cut in shards[1:]:
        factor_of = factor_of * one(*cut)
    return factor_of


def profile(amount, total, most, skew):
    loads = [(1 << 20) // math.isqrt(standing ** skew) + 1 for standing in range(2, amount + 1)]
    rest, counts = total - most - (amount - 1), [1] * (amount - 1)
    while rest > 0:
        free = [i for i in range(amount - 1) if counts[i] < most]
        whole, left = sum([loads[i] for i in free]), rest
        for i in free:
            extra = min(most - counts[i], max(1, left * loads[i] // whole), rest)
            counts[i] = counts[i] + extra
            rest = rest - extra
    return np.array([most] + counts)


def ragged(own_key, number_of, total, most, lean):
    if number_of == 2:
        one = jax.random.randint(own_key, (), max(1, total - most), min(most, total - 1) + 1)
        return jnp.stack([one, total - one])
    sizes = jnp.asarray(profile(number_of, total, most, lean), jnp.int32)
    twos = (number_of - 1) // 2
    source_of, receiver = sizes[1:1 + 2 * twos:2], sizes[2:2 + 2 * twos:2]
    room = jnp.minimum(source_of - 1, most - receiver)
    shifted = jax.random.randint(jax.random.fold_in(own_key, 1), (twos,), 0, 1 << 20) % (room + 1)
    sizes = sizes.at[1:1 + 2 * twos:2].set(source_of - shifted).at[2:2 + 2 * twos:2].set(receiver + shifted)
    return sizes[jax.random.permutation(jax.random.fold_in(own_key, 2), number_of)]


def gaussian(key, dims, deviation, most, split=(), kind=jnp.bfloat16):
    array = jax.random.normal(key, dims, jnp.float32) * deviation
    if len(split) > 0:
        array = levels(key, dims, split, -0.22, 0.18) * array
    return jnp.clip(array, min=-most, max=most).astype(kind)


def noise_with(key, extent, width, reach, pieces, heavy, held_as=jnp.bfloat16):
    drawn = width * jax.random.normal(key, extent, jnp.float32)
    if pieces:
        drawn = drawn * levels(key, extent, pieces, -0.22, 0.18)
    return jnp.clip(raised(drawn, jax.random.fold_in(key, 3), *heavy), -reach, reach).astype(held_as)


def setup_inputs(seed: int = 0) -> dict:
    key_list = jax.random.split(jax.random.key(seed), 6)
    grad_codes = noise_with(key_list[0], (STEPS, REPLICAS, ROWS, FF), 64.0, 448.0, ((1, 32),), (1, 2, 32, 2.75))
    exponents = plant(jax.random.randint(key_list[1], (STEPS, REPLICAS, NB), 7, 11), jax.random.fold_in(key_list[1], 1), 7, 10).astype(jnp.int32)
    accumulated = gaussian(key_list[2], (ROWS, FF), 2.0, 12.0, ((0, 32),))
    arrival = jax.random.permutation(key_list[3], ROWS).astype(jnp.int32)
    bucket_of_row = jnp.searchsorted(jnp.cumsum(ragged(key_list[4], NB, ROWS, BMOST, 1)), jnp.arange(ROWS), side="right").astype(jnp.int32)
    return {"grad_codes": grad_codes, "exponents": exponents, "accumulated": accumulated, "arrival": arrival, "bucket_of_row": bucket_of_row}


epsilon = 1e-6


def reference(grad_codes, exponents, accumulated, arrival, bucket_of_row):
    inverse = jnp.zeros((ROWS,), jnp.int32).at[arrival].set(jnp.arange(ROWS, dtype=jnp.int32))
    member = bucket_of_row[:, None] == jnp.arange(NB, dtype=jnp.int32)[None, :]

    def add_replica(running_sum, replica_item):
        row_block, exponent_row = replica_item
        factor = jnp.exp2(-exponent_row.astype(jnp.float32))
        factor_rows = jnp.sum(jnp.where(member, factor[None, :], jnp.float32(0.0)), axis=1)
        picked = jnp.take(row_block, inverse, axis=0).astype(jnp.float32)
        return running_sum + picked * factor_rows[:, None], None

    running = accumulated
    carried = jnp.zeros((ROWS, FF), jnp.float32)
    unit_list = []
    peak_list = []
    exact_sum = carried
    for micro_step in range(STEPS):
        reduced, _ = lax.scan(add_replica, jnp.zeros((ROWS, FF), jnp.float32),
                              (grad_codes[micro_step], exponents[micro_step]))
        adjusted = reduced - carried
        previous = running.astype(jnp.float32)
        running = lax.optimization_barrier((previous + adjusted).astype(jnp.bfloat16))
        carried = (running.astype(jnp.float32) - previous) - adjusted
        exact_sum = running.astype(jnp.float32) - carried
        row_max = jnp.max(jnp.abs(exact_sum), axis=1)
        peaks = jnp.max(jnp.where(member, row_max[:, None], jnp.float32(0.0)), axis=0)
        peak_rows = jnp.sum(jnp.where(member, peaks[None, :], jnp.float32(0.0)), axis=1)
        unit_list.append((exact_sum / (peak_rows[:, None] + epsilon)).astype(jnp.bfloat16))
        peak_list.append(peaks)
    return jnp.stack(unit_list), jnp.stack(peak_list), exact_sum
```

```python
import functools

import jax
import jax.numpy as jnp
from jax import lax
from jax.experimental import pallas as pl
from jax.experimental.pallas import tpu as pltpu
from jax.sharding import PartitionSpec as P

epsilon = 1e-06
LANES = 128
VMEM_LIMIT = 48 * 1024 * 1024


def bit_orders(bits):
    head = list(range(1, min(4, bits)))
    tail = list(range(1 + len(head), bits))
    return [[0] + head[r:] + head[:r] + tail for r in range(max(1, len(head)))]


def chunks_of(tiles, count):
    plans = {18: PLAN}
    plan = plans.get(tiles, [(1,) * count] * (tiles // count)) if count == 3 else [(tiles,) + (0,) * (count - 1)]
    plan = [list(row) for row in plan]
    plan[0][0] += tiles - sum(map(sum, plan))
    spans, at = [], 0
    for row in plan:
        spans.append([])
        for wide in row:
            spans[-1].append((at * LANES, wide * LANES))
            at += wide
    return spans


PLAN = [(2, 1, 1), (2, 2, 1), (2, 2, 1), (2, 1, 1)]


def exchange(n, orders, spans, codes, exponents_in, accumulated_in, arrival_in, bucket_in, exact, peaks, exponents, accumulated,
             arrival, bucket_of_row, small_sem, x, lhs, begin, out, acc, peak, table, x_sem, send_sem, recv_sem, peak_send, peak_recv, *lands):
    me = lax.axis_index("dp")
    bits = n.bit_length() - 1
    steps, size, width = x.shape
    rows = codes.shape[2]
    groups = size // rows
    half = rows // 2
    small = [
        pltpu.make_async_copy(source, target, small_sem.at[k])
        for k, (source, target) in enumerate(
            [(exponents_in, exponents), (arrival_in, arrival), (bucket_in, bucket_of_row), (accumulated_in, accumulated)]
        )
    ]
    for copy in small:
        copy.start()
    loads = []
    for c, row in enumerate(spans):
        first, wide = row[0][0], sum(w for _, w in row)
        loads.append([])
        for g in range(groups):
            copy = pltpu.make_async_copy(
                codes.at[:, 0, :, pl.ds(g * width + first, wide)],
                x.at[:, pl.ds(g * rows, rows), pl.ds(first, wide)],
                x_sem.at[c, g],
            )
            copy.start()
            loads[-1].append(copy)

    barrier = pltpu.get_barrier_semaphore()

    partners = []
    for b in range(bits):
        stride = 1 << b
        bit = lax.rem(me // stride, 2)
        partners.append(me + stride * (1 - 2 * bit))
    for partner in partners:
        pl.semaphore_signal(barrier, inc=1, device_id={"dp": partner}, device_id_type=pl.DeviceIdType.MESH)

    for copy in small:
        copy.wait()
    slot = lax.broadcasted_iota(jnp.int32, (1, size), 1) % rows
    held = jnp.zeros((1, size), jnp.int32)
    scale = [jnp.zeros((1, size), jnp.int32) for _ in range(steps)]
    for k in range(rows):
        row = arrival[k]
        bucket = bucket_of_row[row]
        here = slot == k
        held = jnp.where(here, row, held)
        for s in range(steps):
            scale[s] = jnp.where(here, exponents[s, 0, bucket], scale[s])
    scale = [jnp.exp2(-e.astype(jnp.float32)) for e in scale]

    row_group = lax.broadcasted_iota(jnp.int32, (size, 1), 0) % groups
    col_group = lax.broadcasted_iota(jnp.int32, (1, size), 1) // rows
    wanted = held * groups + col_group
    place = lax.broadcasted_iota(jnp.int32, (size, 1), 0) // groups
    for q, order in enumerate(orders):
        owner = jnp.zeros_like(place)
        for m, b in enumerate(order):
            bit = (place // (1 << (bits - 1 - m))) % 2
            mine = lax.rem(me // (1 << b), 2)
            owner = owner + ((bit + mine) % 2) * (1 << b)
        mask = owner * groups + row_group == wanted
        for s in range(steps):
            lhs[q, s] = jnp.where(mask, scale[s], 0.0).astype(jnp.bfloat16)
    for g in range(groups):
        begin[g : g + 1, :] = accumulated[:, g * width : (g + 1) * width].astype(jnp.float32)

    def copy_of(c, q, k):
        at, wide = spans[c][q]
        count = half >> k
        cols = pl.ds(at, wide)
        source = out.at[:, :, :, cols] if k == 0 else acc.at[:, pl.ds(count, count), :, cols]
        return pltpu.make_async_remote_copy(
            src_ref=source,
            dst_ref=lands[k].at[:, :, :, cols],
            send_sem=send_sem.at[c, q, k],
            recv_sem=recv_sem.at[c, q, k],
            device_id={"dp": partners[orders[q][k]]},
            device_id_type=pl.DeviceIdType.MESH,
        )

    def stage(c, q, k):
        at, wide = spans[c][q]
        cols = pl.ds(at, wide)
        if k == 0:
            split = half * groups
            for s in range(steps):
                part = jnp.dot(lhs[q, s], x[s, :, cols], preferred_element_type=jnp.float32)
                out[s, :, :, cols] = part[split:].reshape(half, groups, wide)
                acc[s, :, :, cols] = part[:split].reshape(half, groups, wide)
            if c == 0 and q == 0:
                pl.semaphore_wait(barrier, bits)
            copy_of(c, q, 0).start()
            return
        copy_of(c, q, k - 1).wait_recv()
        count = half >> k
        got = lands[k - 1]
        if k < bits:
            acc[:, count : 2 * count, :, cols] += got[:, count : 2 * count, :, cols]
            copy_of(c, q, k).start()
            acc[:, 0:count, :, cols] += got[:, 0:count, :, cols]
        else:
            acc[:, 0:1, :, cols] += got[:, 0:1, :, cols]

    tops = [jnp.zeros((groups, 1), jnp.float32) for _ in range(steps)]
    for wave in range(len(spans) + bits):
        for k in range(bits + 1):
            c = wave - k
            if c < 0 or c >= len(spans):
                continue
            streams = [q for q in range(len(orders)) if spans[c][q][1]]
            if k == 0:
                for copy in loads[c]:
                    copy.wait()
            for q in streams:
                stage(c, q, k)
            if k == bits:
                first, wide = spans[c][0][0], sum(w for _, w in spans[c])
                running = begin[:, first : first + wide]
                carried = jnp.zeros_like(running)
                for s in range(steps):
                    adjusted = acc[s, 0, :, first : first + wide] - carried
                    new = (running + adjusted).astype(jnp.bfloat16).astype(jnp.float32)
                    carried = (new - running) - adjusted
                    running = new
                    total = new - carried
                    tops[s] = jnp.maximum(tops[s], jnp.max(jnp.abs(total), axis=1, keepdims=True))
                    for g in range(groups):
                        exact[s : s + 1, g * width + first : g * width + first + wide] = total[g : g + 1, :]

    lane = lax.broadcasted_iota(jnp.int32, (1, LANES), 1)
    row = jnp.zeros((1, LANES), jnp.float32)
    for s in range(steps):
        row = jnp.where(lane == s, jnp.max(tops[s], axis=0, keepdims=True), row)
    peak[...] = row

    def peak_copy(j):
        return pltpu.make_async_remote_copy(
            src_ref=peak,
            dst_ref=table.at[me],
            send_sem=peak_send.at[j],
            recv_sem=peak_recv.at[j],
            device_id={"dp": lax.rem(me + j, n)},
            device_id_type=pl.DeviceIdType.MESH,
        )

    def tell(j, carry):
        peak_copy(j).start()
        return carry

    def hear(j, carry):
        peak_copy(j).wait()
        return carry

    lax.fori_loop(1, n, tell, 0)
    table[me] = row
    for c in range(len(spans)):
        for q in range(len(orders)):
            if spans[c][q][1]:
                for k in range(bits):
                    copy_of(c, q, k).wait_send()
    lax.fori_loop(1, n, hear, 0)

    for i in range(n):
        peaks[i : i + 1, :] = table[i]


def finish(exact, peaks, bucket_of_row, unit, peak_table, last):
    steps = exact.shape[0]
    buckets = peak_table.shape[1]
    bucket_id = lax.broadcasted_iota(jnp.int32, (buckets, LANES), 0)
    lane_id = lax.broadcasted_iota(jnp.int32, (buckets, LANES), 1)
    by_bucket = jnp.zeros((buckets, LANES), jnp.float32)
    for i in range(peaks.shape[0]):
        by_bucket = jnp.maximum(by_bucket, jnp.where(bucket_id == bucket_of_row[i], peaks[i : i + 1, :], 0.0))
    mine = bucket_of_row[lax.axis_index("dp")]
    own = jnp.max(jnp.where(bucket_id == mine, by_bucket, 0.0), axis=0, keepdims=True)
    for s in range(steps):
        turned = jnp.sum(jnp.where(bucket_id == lane_id, by_bucket[:, s : s + 1], 0.0), axis=0, keepdims=True)
        peak_table[s : s + 1, :] = turned[:, :buckets]
    step_id = lax.broadcasted_iota(jnp.int32, (steps, LANES), 0)
    lane_id = lax.broadcasted_iota(jnp.int32, (steps, LANES), 1)
    scale = jnp.sum(jnp.where(step_id == lane_id, own, 0.0), axis=1, keepdims=True) + epsilon
    unit[...] = (exact[...] / scale).astype(jnp.bfloat16)
    last[...] = exact[steps - 1 :, :]


def on_device(n, tensor, grad_codes, exponents, accumulated, arrival, bucket_of_row):
    steps, _, rows, columns = grad_codes.shape
    buckets = exponents.shape[2]
    bits = n.bit_length() - 1
    groups = max(g for g in (1, 2, 4, 8) if columns % (g * LANES) == 0)
    width = columns // groups
    orders = bit_orders(bits)
    spans = chunks_of(width // LANES, len(orders))
    half = rows // 2
    vmem = pl.BlockSpec(memory_space=pltpu.VMEM)
    smem = pl.BlockSpec(memory_space=pltpu.SMEM)
    operands = (grad_codes, exponents, accumulated, arrival, bucket_of_row)
    exact, peaks = pl.pallas_call(
        functools.partial(exchange, n, orders, spans),
        out_shape=(
            jax.ShapeDtypeStruct((steps, columns), jnp.float32),
            jax.ShapeDtypeStruct((n, LANES), jnp.float32),
        ),
        in_specs=[pl.BlockSpec(memory_space=pltpu.HBM)] * 5,
        out_specs=(vmem, vmem),
        scratch_shapes=[
            pltpu.SMEM(exponents.shape, jnp.int32),
            pltpu.VMEM(accumulated.shape, jnp.bfloat16),
            pltpu.SMEM(arrival.shape, jnp.int32),
            pltpu.SMEM(bucket_of_row.shape, jnp.int32),
            pltpu.SemaphoreType.DMA((4,)),
            pltpu.VMEM((steps, groups * rows, width), jnp.bfloat16),
            pltpu.VMEM((len(orders), steps, groups * rows, groups * rows), jnp.bfloat16),
            pltpu.VMEM((groups, width), jnp.float32),
            pltpu.VMEM((steps, half, groups, width), jnp.float32),
            pltpu.VMEM((steps, half, groups, width), jnp.float32),
            pltpu.VMEM((1, LANES), jnp.float32),
            pltpu.VMEM((n, 1, LANES), jnp.float32),
            pltpu.SemaphoreType.DMA((len(spans), groups)),
            pltpu.SemaphoreType.DMA((len(spans), len(orders), bits)),
            pltpu.SemaphoreType.DMA((len(spans), len(orders), bits)),
            pltpu.SemaphoreType.DMA((n,)),
            pltpu.SemaphoreType.DMA((n,)),
        ]
        + [pltpu.VMEM((steps, half >> k, groups, width), jnp.float32) for k in range(bits)],
        compiler_params=pltpu.CompilerParams(
            collective_id=0, has_side_effects=True, vmem_limit_bytes=VMEM_LIMIT
        ),
    )(*(pltpu.with_memory_space_constraint(a, pltpu.HBM) for a in operands))

    if tensor == 1:
        unit, peak_table, last = pl.pallas_call(
            finish,
            out_shape=(
                jax.ShapeDtypeStruct((steps, columns), jnp.bfloat16),
                jax.ShapeDtypeStruct((steps, buckets), jnp.float32),
                jax.ShapeDtypeStruct((1, columns), jnp.float32),
            ),
            in_specs=[vmem, vmem, smem],
            out_specs=(vmem, vmem, vmem),
            compiler_params=pltpu.CompilerParams(vmem_limit_bytes=8 * 1024 * 1024),
        )(exact, peaks, bucket_of_row)
        return unit.reshape(steps, 1, columns), peak_table, last

    member = bucket_of_row[:, None] == jnp.arange(buckets, dtype=jnp.int32)[None, :]
    by_bucket = jnp.max(jnp.where(member[:, :, None], peaks[:, None, :steps], 0.0), axis=0)
    peak_table = lax.pmax(by_bucket.T, "tensor")
    own = lax.dynamic_slice_in_dim(bucket_of_row, lax.axis_index("dp"), 1, 0)
    own_member = own[:, None] == jnp.arange(buckets, dtype=jnp.int32)[None, :]
    own_peaks = jnp.max(jnp.where(own_member, peak_table, 0.0), axis=1, keepdims=True)
    unit = (exact / (own_peaks + epsilon)).astype(jnp.bfloat16)
    return unit.reshape(steps, 1, columns), peak_table, exact[steps - 1 :]


def solution(mesh):
    return jax.shard_map(
        functools.partial(on_device, mesh.shape["dp"], mesh.shape["tensor"]),
        mesh=mesh,
        in_specs=(P(None, "dp", None, "tensor"), P(None, "dp", None), P("dp", "tensor"), P(), P()),
        out_specs=(P(None, "dp", "tensor"), P(), P("dp", "tensor")),
        check_vma=False,
    )
```

```python
import functools

import jax
import jax.numpy as jnp
from jax import lax
from jax.experimental import pallas as pl
from jax.experimental.pallas import tpu as pltpu
from jax.sharding import PartitionSpec as P

epsilon = 1e-06
LANES = 128
VMEM_LIMIT = 48 * 1024 * 1024

ORDERS = [
    (0, 1, 2, 3, 4), (0, 2, 3, 1, 4), (0, 3, 1, 2, 4), (0, 2, 1, 3, 4),
    (0, 2, 3, 4, 1), (0, 1, 3, 4, 2), (0, 3, 4, 1, 2),
]
UNITS = [
    (0, 1, 0, 4, 6), (1, 1, 0, 4, 3), (2, 1, 0, 4, 5), (3, 1, 0, 4, 2), (4, 1, 0, 4, 1),
    (5, 1, 0, 4, 6), (6, 1, 0, 4, 0), (7, 1, 0, 4, 4), (8, 1, 0, 4, 4), (9, 1, 0, 4, 4),
    (10, 1, 0, 4, 0), (11, 1, 0, 4, 3), (12, 1, 0, 4, 3), (13, 1, 0, 4, 5), (14, 1, 0, 4, 0),
    (15, 1, 0, 4, 0), (16, 1, 0, 4, 0), (17, 1, 0, 4, 0),
]
TURNS = [
    0, 1, 2, 3, 0, 4, 5, 1, 2, 6, 5, 6, 7, 8, 9, 4, 7, 1, 2, 10, 11, 12, 13, 14,
    15, 3, 9, 5, 10, 1, 15, 8, 7, 6, 12, 4, 16, 0, 13, 10, 14, 9, 13, 8, 1, 16, 7, 12,
    11, 2, 17, 9, 10, 13, 6, 15, 17, 16, 12, 10, 8, 3, 4, 11, 14, 0, 15, 1, 16, 6, 7, 17,
    2, 12, 14, 15, 13, 3, 5, 4, 17, 16, 8, 11, 6, 9, 3, 0, 2, 14, 10, 17, 12, 16, 8, 5,
    9, 15, 11, 13, 3, 4, 14, 17, 5, 7, 0, 11,
]
CUTS = (2, 6)


def plan_of(bits, tiles, steps):
    if bits == 5 and tiles == 18 and steps == 4:
        return ORDERS, UNITS, TURNS, CUTS
    head = list(range(1, min(4, bits)))
    tail = list(range(1 + len(head), bits))
    orders = [[0] + head[r:] + head[:r] + tail for r in range(max(1, len(head)))]
    units = [(t, 1, 0, steps, t % len(orders)) for t in range(tiles)]
    turns = [w - k for w in range(tiles + bits) for k in range(bits + 1) if 0 <= w - k < tiles]
    return orders, units, turns, (1,)


def across(b):
    return (1 << b) | (b > 0)


def exchange(n, plan, codes, exponents_in, accumulated_in, arrival_in, bucket_in, exact, peaks, exponents, accumulated,
             arrival, bucket_of_row, small_sem, x, lhs, begin, out, acc, peak, table, x_sem, send_sem, recv_sem,
             peak_send, peak_recv, *lands):
    orders, units, turns, cuts = plan
    me = lax.axis_index("dp")
    bits = n.bit_length() - 1
    steps, size, width = x.shape
    rows = codes.shape[2]
    groups = size // rows
    half = rows // 2
    tiles = width // LANES

    small = [
        pltpu.make_async_copy(source, target, small_sem.at[k])
        for k, (source, target) in enumerate(
            [(arrival_in, arrival), (bucket_in, bucket_of_row), (exponents_in, exponents), (accumulated_in, accumulated)]
        )
    ]
    edges = [0, *(c for c in cuts if c < tiles), tiles]
    loads = []
    for c in range(len(edges) - 1):
        first, wide = edges[c] * LANES, (edges[c + 1] - edges[c]) * LANES
        loads.append(
            [
                pltpu.make_async_copy(
                    codes.at[:, 0, :, pl.ds(g * width + first, wide)],
                    x.at[:, pl.ds(g * rows, rows), pl.ds(first, wide)],
                    x_sem.at[c, g],
                )
                for g in range(groups)
            ]
        )
    for copy in small[:3] + loads[0]:
        copy.start()

    barrier = pltpu.get_barrier_semaphore()
    partners = []
    for b in range(bits):
        partners.append(me ^ across(b))
    for partner in partners:
        pl.semaphore_signal(barrier, inc=1, device_id={"dp": partner}, device_id_type=pl.DeviceIdType.MESH)
    for group in loads[1:]:
        for copy in group:
            copy.start()
    small[3].start()

    for copy in small[:3]:
        copy.wait()
    lane = lax.broadcasted_iota(jnp.int32, (1, size), 1)
    slot = lane & (rows - 1)
    held = jnp.zeros((1, size), jnp.int32)
    scale = [jnp.zeros((1, size), jnp.int32) for _ in range(steps)]
    for k in range(rows):
        row = arrival[k]
        bucket = bucket_of_row[row]
        here = slot == k
        held = jnp.where(here, row, held)
        for s in range(steps):
            scale[s] = jnp.where(here, exponents[s, 0, bucket], scale[s])
    scale = [jnp.exp2(-e.astype(jnp.float32)) for e in scale]
    row_shift = rows.bit_length() - 1
    group_shift = groups.bit_length() - 1
    wanted = ((held ^ me) << group_shift) + (lane >> row_shift)
    line = lax.broadcasted_iota(jnp.int32, (size, 1), 0)

    def spread(q):
        target = line & (groups - 1)
        for m, b in enumerate(orders[q]):
            target = target ^ (((line >> (bits - 1 - m + group_shift)) & 1) * (across(b) << group_shift))
        mask = target == wanted
        for s in range(steps):
            lhs[q, s] = jnp.where(mask, scale[s], 0.0).astype(jnp.bfloat16)

    def copy_of(u, k):
        at, wide, s, count, q = units[u]
        cols, which, part = pl.ds(at * LANES, wide * LANES), pl.ds(s, count), half >> k
        source = out.at[which, :, :, cols] if k == 0 else acc.at[which, pl.ds(part, part), :, cols]
        return pltpu.make_async_remote_copy(
            src_ref=source,
            dst_ref=lands[k].at[which, :, :, cols],
            send_sem=send_sem.at[k],
            recv_sem=recv_sem.at[u, k],
            device_id={"dp": partners[orders[q][k]]},
            device_id_type=pl.DeviceIdType.MESH,
        )

    built, loaded, greeted = set(), 0, False
    done = [0] * len(units)
    left = {}
    for at, wide, *_ in units:
        left[at, wide] = left.get((at, wide), 0) + 1
    tops = [jnp.zeros((groups, LANES), jnp.float32) for _ in range(steps)]
    begun = False
    for u in turns:
        at, wide, s0, count, q = units[u]
        k, done[u] = done[u], done[u] + 1
        first, last, cols = at * LANES, (at + wide) * LANES, pl.ds(at * LANES, wide * LANES)
        which = pl.ds(s0, count)
        if k == 0:
            if q not in built:
                spread(q)
                built.add(q)
            while edges[loaded] < at + wide:
                for copy in loads[loaded]:
                    copy.wait()
                loaded += 1
            split = half * groups
            for s in range(s0, s0 + count):
                product = jnp.dot(lhs[q, s], x[s, :, cols], preferred_element_type=jnp.float32)
                out[s, :, :, cols] = product[split:].reshape(half, groups, last - first)
                acc[s, :, :, cols] = product[:split].reshape(half, groups, last - first)
            if not greeted:
                pl.semaphore_wait(barrier, bits)
                greeted = True
            copy_of(u, 0).start()
            continue
        copy_of(u, k - 1).wait_recv()
        part, got = half >> k, lands[k - 1]
        if k < bits:
            acc[which, part : 2 * part, :, cols] += got[which, part : 2 * part, :, cols]
            copy_of(u, k).start()
            acc[which, 0:part, :, cols] += got[which, 0:part, :, cols]
            continue
        acc[which, 0:1, :, cols] += got[which, 0:1, :, cols]
        left[at, wide] -= 1
        if left[at, wide]:
            continue
        if not begun:
            small[3].wait()
            for g in range(groups):
                begin[g : g + 1, :] = accumulated[:, g * width : (g + 1) * width].astype(jnp.float32)
            begun = True
        running = begin[:, first:last]
        carried = jnp.zeros_like(running)
        for s in range(steps):
            adjusted = acc[s, 0, :, first:last] - carried
            new = (running + adjusted).astype(jnp.bfloat16).astype(jnp.float32)
            carried = (new - running) - adjusted
            running = new
            total = new - carried
            for t in range(wide):
                tops[s] = jnp.maximum(tops[s], jnp.abs(total[:, t * LANES : (t + 1) * LANES]))
            for g in range(groups):
                exact[s : s + 1, g * width + first : g * width + last] = total[g : g + 1, :]

    lane = lax.broadcasted_iota(jnp.int32, (1, LANES), 1)
    row = jnp.zeros((1, LANES), jnp.float32)
    for s in range(steps):
        top = jnp.max(jnp.max(tops[s], axis=0, keepdims=True), axis=1, keepdims=True)
        row = jnp.where(lane == s, top, row)
    peak[...] = row

    def everything(source, target, sent, received, device):
        return pltpu.make_async_remote_copy(
            src_ref=source,
            dst_ref=target,
            send_sem=sent,
            recv_sem=received,
            device_id={"dp": device},
            device_id_type=pl.DeviceIdType.MESH,
        )

    def peak_copy(j):
        return pltpu.make_async_remote_copy(
            src_ref=peak,
            dst_ref=table.at[me],
            send_sem=peak_send,
            recv_sem=peak_recv,
            device_id={"dp": lax.rem(me + j, n)},
            device_id_type=pl.DeviceIdType.MESH,
        )

    def tell(j, carry):
        peak_copy(j).start()
        return carry

    lax.fori_loop(1, n, tell, 0)
    table[me] = row
    for k in range(bits):
        everything(lands[k], lands[k], send_sem.at[k], recv_sem.at[0, 0], partners[0]).wait_send()
    others = everything(table.at[pl.ds(1, n - 1)], table.at[pl.ds(1, n - 1)], peak_send, peak_recv, partners[0])
    others.wait_send()
    others.wait_recv()
    for i in range(n):
        peaks[i : i + 1, :] = table[i]


def finish(exact, peaks, bucket_of_row, unit, peak_table, last):
    steps = exact.shape[0]
    buckets = peak_table.shape[1]
    bucket_id = lax.broadcasted_iota(jnp.int32, (buckets, LANES), 0)
    lane_id = lax.broadcasted_iota(jnp.int32, (buckets, LANES), 1)
    by_bucket = jnp.zeros((buckets, LANES), jnp.float32)
    for i in range(peaks.shape[0]):
        by_bucket = jnp.maximum(by_bucket, jnp.where(bucket_id == bucket_of_row[i], peaks[i : i + 1, :], 0.0))
    mine = bucket_of_row[lax.axis_index("dp")]
    own = jnp.max(jnp.where(bucket_id == mine, by_bucket, 0.0), axis=0, keepdims=True)
    for s in range(steps):
        turned = jnp.sum(jnp.where(bucket_id == lane_id, by_bucket[:, s : s + 1], 0.0), axis=0, keepdims=True)
        peak_table[s : s + 1, :] = turned[:, :buckets]
    step_id = lax.broadcasted_iota(jnp.int32, (steps, LANES), 0)
    lane_id = lax.broadcasted_iota(jnp.int32, (steps, LANES), 1)
    scale = jnp.sum(jnp.where(step_id == lane_id, own, 0.0), axis=1, keepdims=True) + epsilon
    unit[...] = (exact[...] / scale).astype(jnp.bfloat16)
    last[...] = exact[steps - 1 :, :]


def on_device(n, tensor, grad_codes, exponents, accumulated, arrival, bucket_of_row):
    steps, _, rows, columns = grad_codes.shape
    buckets = exponents.shape[2]
    bits = n.bit_length() - 1
    groups = max(g for g in (1, 2, 4, 8) if columns % (g * LANES) == 0)
    width = columns // groups
    plan = plan_of(bits, width // LANES, steps)
    orders, units, _, cuts = plan
    half = rows // 2
    vmem = pl.BlockSpec(memory_space=pltpu.VMEM)
    smem = pl.BlockSpec(memory_space=pltpu.SMEM)
    operands = (grad_codes, exponents, accumulated, arrival, bucket_of_row)
    exact, peaks = pl.pallas_call(
        functools.partial(exchange, n, plan),
        out_shape=(
            jax.ShapeDtypeStruct((steps, columns), jnp.float32),
            jax.ShapeDtypeStruct((n, LANES), jnp.float32),
        ),
        in_specs=[pl.BlockSpec(memory_space=pltpu.HBM)] * 5,
        out_specs=(vmem, vmem),
        scratch_shapes=[
            pltpu.SMEM(exponents.shape, jnp.int32),
            pltpu.VMEM(accumulated.shape, jnp.bfloat16),
            pltpu.SMEM(arrival.shape, jnp.int32),
            pltpu.SMEM(bucket_of_row.shape, jnp.int32),
            pltpu.SemaphoreType.DMA((4,)),
            pltpu.VMEM((steps, groups * rows, width), jnp.bfloat16),
            pltpu.VMEM((len(orders), steps, groups * rows, groups * rows), jnp.bfloat16),
            pltpu.VMEM((groups, width), jnp.float32),
            pltpu.VMEM((steps, half, groups, width), jnp.float32),
            pltpu.VMEM((steps, half, groups, width), jnp.float32),
            pltpu.VMEM((1, LANES), jnp.float32),
            pltpu.VMEM((n, 1, LANES), jnp.float32),
            pltpu.SemaphoreType.DMA((len(cuts) + 1, groups)),
            pltpu.SemaphoreType.DMA((bits,)),
            pltpu.SemaphoreType.DMA((len(units), bits)),
            pltpu.SemaphoreType.DMA,
            pltpu.SemaphoreType.DMA,
        ]
        + [pltpu.VMEM((steps, half >> k, groups, width), jnp.float32) for k in range(bits)],
        compiler_params=pltpu.CompilerParams(
            collective_id=0, has_side_effects=True, vmem_limit_bytes=VMEM_LIMIT
        ),
    )(*(pltpu.with_memory_space_constraint(a, pltpu.HBM) for a in operands))

    if tensor == 1:
        unit, peak_table, last = pl.pallas_call(
            finish,
            out_shape=(
                jax.ShapeDtypeStruct((steps, columns), jnp.bfloat16),
                jax.ShapeDtypeStruct((steps, buckets), jnp.float32),
                jax.ShapeDtypeStruct((1, columns), jnp.float32),
            ),
            in_specs=[vmem, vmem, smem],
            out_specs=(vmem, vmem, vmem),
            compiler_params=pltpu.CompilerParams(vmem_limit_bytes=8 * 1024 * 1024),
        )(exact, peaks, bucket_of_row)
        return unit.reshape(steps, 1, columns), peak_table, last

    member = bucket_of_row[:, None] == jnp.arange(buckets, dtype=jnp.int32)[None, :]
    by_bucket = jnp.max(jnp.where(member[:, :, None], peaks[:, None, :steps], 0.0), axis=0)
    peak_table = lax.pmax(by_bucket.T, "tensor")
    own = lax.dynamic_slice_in_dim(bucket_of_row, lax.axis_index("dp"), 1, 0)
    own_member = own[:, None] == jnp.arange(buckets, dtype=jnp.int32)[None, :]
    own_peaks = jnp.max(jnp.where(own_member, peak_table, 0.0), axis=1, keepdims=True)
    unit = (exact / (own_peaks + epsilon)).astype(jnp.bfloat16)
    return unit.reshape(steps, 1, columns), peak_table, exact[steps - 1 :]


def solution(mesh):
    return jax.shard_map(
        functools.partial(on_device, mesh.shape["dp"], mesh.shape["tensor"]),
        mesh=mesh,
        in_specs=(P(None, "dp", None, "tensor"), P(None, "dp", None), P("dp", "tensor"), P(), P()),
        out_specs=(P(None, "dp", "tensor"), P(), P("dp", "tensor")),
        check_vma=False,
    )
```

```python
import functools

import jax
import jax.numpy as jnp
from jax import lax
from jax.experimental import pallas as pl
from jax.experimental.pallas import tpu as pltpu
from jax.sharding import PartitionSpec as P

epsilon = 1e-06
LANES = 128
VMEM_LIMIT = 48 * 1024 * 1024

ORDERS = [
    (0, 2, 3, 1, 4), (0, 2, 1, 3, 4), (0, 1, 3, 4, 2), (0, 3, 2, 1, 4),
    (0, 3, 4, 2, 1),
]
UNITS = [
    (0, 1, 0, 2, 4), (1, 1, 0, 2, 2), (1, 1, 2, 2, 1), (2, 1, 0, 4, 2), (3, 1, 0, 4, 4),
    (4, 1, 0, 4, 1), (0, 1, 2, 2, 2), (5, 1, 0, 4, 1), (6, 1, 0, 4, 1), (7, 1, 0, 4, 2),
    (8, 1, 0, 4, 1), (9, 1, 0, 4, 0), (10, 1, 0, 4, 2), (11, 1, 0, 2, 3), (12, 1, 0, 2, 3),
    (13, 1, 0, 2, 1), (14, 1, 0, 4, 1), (13, 1, 2, 2, 1), (11, 1, 2, 2, 1), (15, 1, 0, 4, 2),
    (16, 1, 0, 4, 2), (12, 1, 2, 2, 1), (17, 1, 0, 2, 1), (17, 1, 2, 2, 1),
]
TURNS = [
    0, 1, 2, 3, 4, 5, 0, 1, 6, 2, 7, 8, 3, 9, 4, 5, 10, 6, 11, 7, 12, 8, 13, 9,
    14, 0, 15, 10, 16, 1, 2, 11, 17, 18, 12, 19, 13, 14, 20, 15, 21, 16, 22, 17, 23, 18, 19, 3,
    20, 21, 5, 22, 4, 23, 0, 1, 6, 13, 7, 9, 2, 14, 8, 4, 1, 3, 12, 6, 10, 9, 2, 19,
    3, 11, 6, 12, 15, 20, 9, 2, 19, 5, 16, 7, 11, 12, 17, 8, 19, 18, 20, 10, 5, 15, 21, 7,
    8, 16, 22, 11, 10, 17, 20, 23, 15, 0, 18, 5, 13, 21, 7, 16, 14, 22, 8, 17, 4, 23, 1, 11,
    0, 3, 18, 6, 13, 10, 21, 9, 15, 12, 14, 19, 22, 20, 4, 23, 16, 17, 13, 18, 21, 14, 22, 23,
]
CUTS = (2, 6)


def plan_of(bits, tiles, steps):
    if bits == 5 and tiles == 18 and steps == 4:
        return ORDERS, UNITS, TURNS, CUTS
    head = list(range(1, min(4, bits)))
    tail = list(range(1 + len(head), bits))
    orders = [[0] + head[r:] + head[:r] + tail for r in range(max(1, len(head)))]
    units = [(t, 1, 0, steps, t % len(orders)) for t in range(tiles)]
    turns = [w - k for w in range(tiles + bits) for k in range(bits + 1) if 0 <= w - k < tiles]
    return orders, units, turns, (1,)


def slots_of(plan, bits):
    orders, units, turns, _ = plan
    seen, start, wait = [0] * len(units), {}, {}
    for at, u in enumerate(turns):
        k, seen[u] = seen[u], seen[u] + 1
        if k < bits:
            start[u, k] = at
        if k > 0:
            wait[u, k - 1] = at
    dim = {c: orders[units[c[0]][4]][c[1]] for c in start}
    slots, held = {}, []
    for c in sorted(start, key=start.get):
        there = [v for v in start if dim[v] == dim[c] and wait[v] <= start[c]]
        latest = max((start[v] for v in there), default=-1)
        for slot, last in enumerate(held):
            if wait[last] <= latest:
                slots[c], held[slot] = slot, c
                break
        else:
            slots[c] = len(held)
            held.append(c)
    return slots


def across(b):
    return (1 << b) | (b > 0)


def exchange(n, plan, codes, exponents_in, accumulated_in, arrival_in, bucket_in, exact, last_row, peak_table, scales, exponents,
             accumulated, arrival, bucket_of_row, small_sem, x, lhs, begin, out, acc, peak, table, x_sem, send_sem, recv_sem,
             peak_send, peak_recv, *lands):
    orders, units, turns, cuts = plan
    slots = slots_of(plan, n.bit_length() - 1)
    me = lax.axis_index("dp")
    bits = n.bit_length() - 1
    steps, size, width = x.shape
    rows = codes.shape[2]
    groups = size // rows
    half = rows // 2
    tiles = width // LANES

    small = [
        pltpu.make_async_copy(source, target, small_sem.at[k])
        for k, (source, target) in enumerate(
            [(arrival_in, arrival), (bucket_in, bucket_of_row), (exponents_in, exponents), (accumulated_in, accumulated)]
        )
    ]
    edges = [0, *(c for c in cuts if c < tiles), tiles]
    loads = []
    for c in range(len(edges) - 1):
        first, wide = edges[c] * LANES, (edges[c + 1] - edges[c]) * LANES
        loads.append(
            [
                pltpu.make_async_copy(
                    codes.at[:, 0, :, pl.ds(g * width + first, wide)],
                    x.at[:, pl.ds(g * rows, rows), pl.ds(first, wide)],
                    x_sem.at[c],
                )
                for g in range(groups)
            ]
        )
    for copy in small[:3] + loads[0]:
        copy.start()

    barrier = pltpu.get_barrier_semaphore()
    partners = []
    for b in range(bits):
        partners.append(me ^ across(b))
    for partner in partners:
        pl.semaphore_signal(barrier, inc=1, device_id={"dp": partner}, device_id_type=pl.DeviceIdType.MESH)
    for group in loads[1:]:
        for copy in group:
            copy.start()
    small[3].start()

    for copy in small[:3]:
        copy.wait()
    lane = lax.broadcasted_iota(jnp.int32, (1, size), 1)
    slot = lane & (rows - 1)
    held = jnp.zeros((1, size), jnp.int32)
    scale = [jnp.zeros((1, size), jnp.int32) for _ in range(steps)]
    for k in range(rows):
        row = arrival[k]
        bucket = bucket_of_row[row]
        here = slot == k
        held = jnp.where(here, row, held)
        for s in range(steps):
            scale[s] = jnp.where(here, exponents[s, 0, bucket], scale[s])
    scale = [jnp.exp2(-e.astype(jnp.float32)) for e in scale]
    row_shift = rows.bit_length() - 1
    group_shift = groups.bit_length() - 1
    wanted = ((held ^ me) << group_shift) + (lane >> row_shift)
    line = lax.broadcasted_iota(jnp.int32, (size, 1), 0)

    def spread(q, wanted_steps):
        target = line & (groups - 1)
        for m, b in enumerate(orders[q]):
            target = target ^ (((line >> (bits - 1 - m + group_shift)) & 1) * (across(b) << group_shift))
        mask = target == wanted
        for s in wanted_steps:
            lhs[q, s] = jnp.where(mask, scale[s], 0.0).astype(jnp.bfloat16)

    def copy_of(u, k):
        at, wide, s, count, q = units[u]
        cols, which, part = pl.ds(at * LANES, wide * LANES), pl.ds(s, count), half >> k
        source = out.at[which, :, :, cols] if k == 0 else acc.at[which, pl.ds(part, part), :, cols]
        return pltpu.make_async_remote_copy(
            src_ref=source,
            dst_ref=lands[k].at[which, :, :, cols],
            send_sem=send_sem.at[k],
            recv_sem=recv_sem.at[slots[u, k]],
            device_id={"dp": partners[orders[q][k]]},
            device_id_type=pl.DeviceIdType.MESH,
        )

    built, loaded, greeted = set(), 0, False
    done = [0] * len(units)
    left = {}
    for at, wide, *_ in units:
        left[at, wide] = left.get((at, wide), 0) + 1
    tops = [jnp.zeros((groups, LANES), jnp.float32) for _ in range(steps)]
    begun = False
    for u in turns:
        at, wide, s0, count, q = units[u]
        k, done[u] = done[u], done[u] + 1
        first, last, cols = at * LANES, (at + wide) * LANES, pl.ds(at * LANES, wide * LANES)
        which = pl.ds(s0, count)
        if k == 0:
            missing = [s for s in range(s0, s0 + count) if (q, s) not in built]
            if missing:
                spread(q, missing)
                built.update((q, s) for s in missing)
            while edges[loaded] < at + wide:
                chunk = x.at[:, :, pl.ds(edges[loaded] * LANES, (edges[loaded + 1] - edges[loaded]) * LANES)]
                pltpu.make_async_copy(chunk, chunk, x_sem.at[loaded]).wait()
                loaded += 1
            split = half * groups
            for s in range(s0, s0 + count):
                product = jnp.dot(lhs[q, s], x[s, :, cols], preferred_element_type=jnp.float32)
                out[s, :, :, cols] = product[split:].reshape(half, groups, last - first)
                acc[s, :, :, cols] = product[:split].reshape(half, groups, last - first)
            if not greeted:
                pl.semaphore_wait(barrier, bits)
                greeted = True
            copy_of(u, 0).start()
            continue
        copy_of(u, k - 1).wait_recv()
        part, got = half >> k, lands[k - 1]
        if k < bits:
            acc[which, part : 2 * part, :, cols] += got[which, part : 2 * part, :, cols]
            copy_of(u, k).start()
            acc[which, 0:part, :, cols] += got[which, 0:part, :, cols]
            continue
        acc[which, 0:1, :, cols] += got[which, 0:1, :, cols]
        left[at, wide] -= 1
        if left[at, wide]:
            continue
        if not begun:
            small[3].wait()
            for g in range(groups):
                begin[g : g + 1, :] = accumulated[:, g * width : (g + 1) * width].astype(jnp.float32)
            begun = True
        running = begin[:, first:last]
        carried = jnp.zeros_like(running)
        for s in range(steps):
            adjusted = acc[s, 0, :, first:last] - carried
            new = (running + adjusted).astype(jnp.bfloat16).astype(jnp.float32)
            carried = (new - running) - adjusted
            running = new
            total = new - carried
            for t in range(wide):
                tops[s] = jnp.maximum(tops[s], jnp.abs(total[:, t * LANES : (t + 1) * LANES]))
            for g in range(groups):
                exact[s : s + 1, g * width + first : g * width + last] = total[g : g + 1, :]
        for g in range(groups):
            last_row[:, g * width + first : g * width + last] = total[g : g + 1, :]

    lane = lax.broadcasted_iota(jnp.int32, (1, LANES), 1)
    row = jnp.zeros((1, LANES), jnp.float32)
    for s in range(steps):
        top = jnp.max(jnp.max(tops[s], axis=0, keepdims=True), axis=1, keepdims=True)
        row = jnp.where(lane == s, top, row)
    peak[...] = row

    def everything(source, target, sent, received, device):
        return pltpu.make_async_remote_copy(
            src_ref=source,
            dst_ref=target,
            send_sem=sent,
            recv_sem=received,
            device_id={"dp": device},
            device_id_type=pl.DeviceIdType.MESH,
        )

    def peak_copy(j):
        return pltpu.make_async_remote_copy(
            src_ref=peak,
            dst_ref=table.at[me],
            send_sem=peak_send,
            recv_sem=peak_recv,
            device_id={"dp": me ^ (n - j)},
            device_id_type=pl.DeviceIdType.MESH,
        )

    def tell(j, carry):
        peak_copy(j).start()
        return carry

    lax.fori_loop(1, n, tell, 0)
    table[me] = row
    for k in range(bits):
        everything(lands[k], lands[k], send_sem.at[k], recv_sem.at[0], partners[0]).wait_send()
    others = everything(table.at[pl.ds(1, n - 1)], table.at[pl.ds(1, n - 1)], peak_send, peak_recv, partners[0])
    others.wait_send()
    others.wait_recv()
    buckets = exponents.shape[2]
    bucket_id = lax.broadcasted_iota(jnp.int32, (buckets, LANES), 0)
    lane_id = lax.broadcasted_iota(jnp.int32, (buckets, LANES), 1)
    by_bucket = jnp.zeros((buckets, LANES), jnp.float32)
    for i in range(n):
        by_bucket = jnp.maximum(by_bucket, jnp.where(bucket_id == bucket_of_row[i], table[i], 0.0))
    own = jnp.max(jnp.where(bucket_id == bucket_of_row[me], by_bucket, 0.0), axis=0, keepdims=True)
    for s in range(steps):
        turned = jnp.sum(jnp.where(bucket_id == lane_id, by_bucket[:, s : s + 1], 0.0), axis=0, keepdims=True)
        peak_table[s : s + 1, :] = turned[:, :buckets]
        scales[s : s + 1, :] = 1.0 / (jnp.broadcast_to(own[:, s : s + 1], (1, LANES)) + epsilon)


def finish(exact, last_row, peaks, scales, unit, peak_table, last, codes, sem):
    columns = exact.shape[1]
    copies = [
        pltpu.make_async_copy(last_row, last, sem.at[0]),
        pltpu.make_async_copy(peaks, peak_table, sem.at[1]),
    ]
    for copy in copies:
        copy.start()
    scale = scales[:, :1]
    half = columns // 2
    for h in range(2):
        part = pl.ds(h * half, half)
        codes[:, part] = (exact[:, part] * scale).astype(jnp.bfloat16)
        copies.append(pltpu.make_async_copy(codes.at[:, part], unit.at[:, part], sem.at[2 + h]))
        copies[-1].start()
    for copy in copies:
        copy.wait()


def on_device(n, tensor, grad_codes, exponents, accumulated, arrival, bucket_of_row):
    steps, _, rows, columns = grad_codes.shape
    buckets = exponents.shape[2]
    bits = n.bit_length() - 1
    groups = max(g for g in (1, 2, 4, 8) if columns % (g * LANES) == 0)
    width = columns // groups
    plan = plan_of(bits, width // LANES, steps)
    orders, units, _, cuts = plan
    half = rows // 2
    vmem = pl.BlockSpec(memory_space=pltpu.VMEM)
    operands = (grad_codes, exponents, accumulated, arrival, bucket_of_row)
    exact, last_row, peaks, scales = pl.pallas_call(
        functools.partial(exchange, n, plan),
        out_shape=(
            jax.ShapeDtypeStruct((steps, columns), jnp.float32),
            jax.ShapeDtypeStruct((1, columns), jnp.float32),
            jax.ShapeDtypeStruct((steps, buckets), jnp.float32),
            jax.ShapeDtypeStruct((steps, LANES), jnp.float32),
        ),
        in_specs=[pl.BlockSpec(memory_space=pltpu.HBM)] * 5,
        out_specs=(vmem,) * 4,
        scratch_shapes=[
            pltpu.SMEM(exponents.shape, jnp.int32),
            pltpu.VMEM(accumulated.shape, jnp.bfloat16),
            pltpu.SMEM(arrival.shape, jnp.int32),
            pltpu.SMEM(bucket_of_row.shape, jnp.int32),
            pltpu.SemaphoreType.DMA((4,)),
            pltpu.VMEM((steps, groups * rows, width), jnp.bfloat16),
            pltpu.VMEM((len(orders), steps, groups * rows, groups * rows), jnp.bfloat16),
            pltpu.VMEM((groups, width), jnp.float32),
            pltpu.VMEM((steps, half, groups, width), jnp.float32),
            pltpu.VMEM((steps, half, groups, width), jnp.float32),
            pltpu.VMEM((1, LANES), jnp.float32),
            pltpu.VMEM((n, 1, LANES), jnp.float32),
            pltpu.SemaphoreType.DMA((len(cuts) + 1,)),
            pltpu.SemaphoreType.DMA((bits,)),
            pltpu.SemaphoreType.DMA((max(slots_of(plan, bits).values()) + 1,)),
            pltpu.SemaphoreType.DMA,
            pltpu.SemaphoreType.DMA,
        ]
        + [pltpu.VMEM((steps, half >> k, groups, width), jnp.float32) for k in range(bits)],
        compiler_params=pltpu.CompilerParams(
            collective_id=0, has_side_effects=True, vmem_limit_bytes=VMEM_LIMIT
        ),
    )(*(pltpu.with_memory_space_constraint(a, pltpu.HBM) for a in operands))

    if tensor == 1:
        unit, peak_table, last = pl.pallas_call(
            finish,
            out_shape=(
                jax.ShapeDtypeStruct((steps, columns), jnp.bfloat16),
                jax.ShapeDtypeStruct((steps, buckets), jnp.float32),
                jax.ShapeDtypeStruct((1, columns), jnp.float32),
            ),
            in_specs=[vmem] * 4,
            out_specs=(pl.BlockSpec(memory_space=pltpu.HBM),) * 3,
            scratch_shapes=[pltpu.VMEM((steps, columns), jnp.bfloat16), pltpu.SemaphoreType.DMA((4,))],
            compiler_params=pltpu.CompilerParams(vmem_limit_bytes=8 * 1024 * 1024),
        )(exact, last_row, peaks, scales)
        return unit.reshape(steps, 1, columns), peak_table, last

    peak_table = lax.pmax(peaks, "tensor")
    own = lax.dynamic_slice_in_dim(bucket_of_row, lax.axis_index("dp"), 1, 0)
    own_member = own[:, None] == jnp.arange(buckets, dtype=jnp.int32)[None, :]
    own_peaks = jnp.max(jnp.where(own_member, peak_table, 0.0), axis=1, keepdims=True)
    unit = (exact / (own_peaks + epsilon)).astype(jnp.bfloat16)
    return unit.reshape(steps, 1, columns), peak_table, last_row


def solution(mesh):
    return jax.shard_map(
        functools.partial(on_device, mesh.shape["dp"], mesh.shape["tensor"]),
        mesh=mesh,
        in_specs=(P(None, "dp", None, "tensor"), P(None, "dp", None), P("dp", "tensor"), P(), P()),
        out_specs=(P(None, "dp", "tensor"), P(), P("dp", "tensor")),
        check_vma=False,
    )
```

```python
import functools

import jax
import jax.numpy as jnp
from jax import lax
from jax.experimental import pallas as pl
from jax.experimental.pallas import tpu as pltpu
from jax.sharding import PartitionSpec as P

epsilon = 1e-06
LANES = 128
VMEM_LIMIT = 48 * 1024 * 1024

ORDERS = [
    (0, 1, 2, 3, 4), (0, 2, 3, 1, 4), (0, 3, 1, 2, 4), (0, 2, 1, 3, 4),
    (0, 2, 3, 4, 1), (0, 3, 4, 1, 2), (0, 1, 3, 2, 4), (0, 3, 2, 4, 1),
    (0, 3, 4, 2, 1),
]
UNITS = [
    (0, 1, 0, 2, 8), (1, 1, 0, 2, 4), (2, 1, 0, 4, 0), (3, 1, 0, 2, 7), (4, 1, 0, 4, 3),
    (5, 1, 0, 2, 1), (6, 1, 0, 4, 8), (7, 1, 0, 4, 1), (0, 1, 2, 2, 8), (8, 1, 0, 4, 5),
    (9, 1, 0, 4, 0), (10, 1, 0, 4, 0), (11, 1, 0, 4, 2), (12, 1, 0, 4, 0), (13, 1, 0, 4, 3),
    (14, 1, 0, 4, 3), (1, 1, 2, 2, 3), (15, 1, 0, 4, 0), (3, 1, 2, 2, 0), (5, 1, 2, 2, 0),
    (16, 1, 0, 4, 3), (17, 1, 0, 4, 6),
]
TURNS = [
    0, 1, 2, 3, 4, 0, 1, 5, 6, 2, 7, 3, 8, 9, 4, 10, 11, 6, 12, 10, 13, 7, 14, 15,
    8, 13, 16, 1, 16, 17, 4, 18, 9, 19, 15, 12, 6, 20, 10, 3, 11, 18, 21, 16, 0, 20, 4, 13,
    15, 9, 10, 11, 21, 14, 7, 3, 17, 8, 15, 20, 16, 19, 12, 18, 5, 10, 13, 2, 4, 21, 15, 11,
    14, 18, 16, 17, 13, 7, 20, 5, 21, 1, 3, 11, 19, 15, 2, 12, 6, 18, 8, 17, 9, 0, 20, 14,
    21, 5, 7, 19, 2, 12, 17, 5, 20, 10, 14, 0, 19, 1, 6, 9, 8, 16, 1, 21, 13, 9, 3, 18,
    2, 4, 12, 14, 6, 7, 11, 8, 17, 0, 5, 19,
]
CUTS = (2, 6)


def plan_of(bits, tiles, steps):
    if bits == 5 and tiles == 18 and steps == 4:
        return ORDERS, UNITS, TURNS, CUTS
    head = list(range(1, min(4, bits)))
    tail = list(range(1 + len(head), bits))
    orders = [[0] + head[r:] + head[:r] + tail for r in range(max(1, len(head)))]
    units = [(t, 1, 0, steps, t % len(orders)) for t in range(tiles)]
    turns = [w - k for w in range(tiles + bits) for k in range(bits + 1) if 0 <= w - k < tiles]
    return orders, units, turns, (1,)


def slots_of(plan, bits):
    orders, units, turns, _ = plan
    seen, start, wait = [0] * len(units), {}, {}
    for at, u in enumerate(turns):
        k, seen[u] = seen[u], seen[u] + 1
        if k < bits:
            start[u, k] = at
        if k > 0:
            wait[u, k - 1] = at
    dim = {c: orders[units[c[0]][4]][c[1]] for c in start}
    slots, held = {}, []
    for c in sorted(start, key=start.get):
        there = [v for v in start if dim[v] == dim[c] and wait[v] <= start[c]]
        latest = max((start[v] for v in there), default=-1)
        for slot, last in enumerate(held):
            if wait[last] <= latest:
                slots[c], held[slot] = slot, c
                break
        else:
            slots[c] = len(held)
            held.append(c)
    return slots


def across(b):
    return (1 << b) | (b > 0)


def exchange(n, plan, codes, exponents_in, accumulated_in, arrival_in, bucket_in, exact, last_row, peak_table, scales, exponents,
             accumulated, arrival, bucket_of_row, small_sem, x, lhs, begin, out, acc, peak, table, x_sem, send_sem, recv_sem,
             peak_send, peak_recv, *lands):
    orders, units, turns, cuts = plan
    slots = slots_of(plan, n.bit_length() - 1)
    me = lax.axis_index("dp")
    bits = n.bit_length() - 1
    steps, size, width = x.shape
    rows = codes.shape[2]
    groups = size // rows
    half = rows // 2
    tiles = width // LANES

    small = [
        pltpu.make_async_copy(source, target, small_sem.at[k])
        for k, (source, target) in enumerate(
            [(arrival_in, arrival), (bucket_in, bucket_of_row), (exponents_in, exponents), (accumulated_in, accumulated)]
        )
    ]
    edges = [0, *(c for c in cuts if c < tiles), tiles]
    loads = []
    for c in range(len(edges) - 1):
        first, wide = edges[c] * LANES, (edges[c + 1] - edges[c]) * LANES
        loads.append(
            [
                pltpu.make_async_copy(
                    codes.at[:, 0, :, pl.ds(g * width + first, wide)],
                    x.at[:, pl.ds(g * rows, rows), pl.ds(first, wide)],
                    x_sem.at[c],
                )
                for g in range(groups)
            ]
        )
    for copy in small[:3] + loads[0]:
        copy.start()

    barrier = pltpu.get_barrier_semaphore()
    partners = []
    for b in range(bits):
        partners.append(me ^ across(b))
    for partner in partners:
        pl.semaphore_signal(barrier, inc=1, device_id={"dp": partner}, device_id_type=pl.DeviceIdType.MESH)
    for group in loads[1:]:
        for copy in group:
            copy.start()
    small[3].start()

    for copy in small[:3]:
        copy.wait()
    lane = lax.broadcasted_iota(jnp.int32, (1, size), 1)
    slot = lane & (rows - 1)
    held = jnp.zeros((1, size), jnp.int32)
    scale = [jnp.zeros((1, size), jnp.int32) for _ in range(steps)]
    for k in range(rows):
        row = arrival[k]
        bucket = bucket_of_row[row]
        here = slot == k
        held = jnp.where(here, row, held)
        for s in range(steps):
            scale[s] = jnp.where(here, exponents[s, 0, bucket], scale[s])
    scale = [jnp.exp2(-e.astype(jnp.float32)) for e in scale]
    row_shift = rows.bit_length() - 1
    group_shift = groups.bit_length() - 1
    wanted = ((held ^ me) << group_shift) + (lane >> row_shift)
    line = lax.broadcasted_iota(jnp.int32, (size, 1), 0)

    def spread(q, wanted_steps):
        target = line & (groups - 1)
        for m, b in enumerate(orders[q]):
            target = target ^ (((line >> (bits - 1 - m + group_shift)) & 1) * (across(b) << group_shift))
        mask = target == wanted
        for s in wanted_steps:
            lhs[q, s] = jnp.where(mask, scale[s], 0.0).astype(jnp.bfloat16)

    def copy_of(u, k):
        at, wide, s, count, q = units[u]
        cols, which, part = pl.ds(at * LANES, wide * LANES), pl.ds(s, count), half >> k
        source = out.at[which, :, :, cols] if k == 0 else acc.at[which, pl.ds(part, part), :, cols]
        return pltpu.make_async_remote_copy(
            src_ref=source,
            dst_ref=lands[k].at[which, :, :, cols],
            send_sem=send_sem.at[k],
            recv_sem=recv_sem.at[slots[u, k]],
            device_id={"dp": partners[orders[q][k]]},
            device_id_type=pl.DeviceIdType.MESH,
        )

    built, loaded, greeted = set(), 0, False
    done = [0] * len(units)
    left = {}
    for at, wide, *_ in units:
        left[at, wide] = left.get((at, wide), 0) + 1
    tops = [jnp.zeros((groups, LANES), jnp.float32) for _ in range(steps)]
    begun = False
    for u in turns:
        at, wide, s0, count, q = units[u]
        k, done[u] = done[u], done[u] + 1
        first, last, cols = at * LANES, (at + wide) * LANES, pl.ds(at * LANES, wide * LANES)
        which = pl.ds(s0, count)
        if k == 0:
            missing = [s for s in range(s0, s0 + count) if (q, s) not in built]
            if missing:
                spread(q, missing)
                built.update((q, s) for s in missing)
            while edges[loaded] < at + wide:
                chunk = x.at[:, :, pl.ds(edges[loaded] * LANES, (edges[loaded + 1] - edges[loaded]) * LANES)]
                pltpu.make_async_copy(chunk, chunk, x_sem.at[loaded]).wait()
                loaded += 1
            split = half * groups
            for s in range(s0, s0 + count):
                product = jnp.dot(lhs[q, s], x[s, :, cols], preferred_element_type=jnp.float32)
                out[s, :, :, cols] = product[split:].reshape(half, groups, last - first)
                acc[s, :, :, cols] = product[:split].reshape(half, groups, last - first)
            if not greeted:
                pl.semaphore_wait(barrier, bits)
                greeted = True
            copy_of(u, 0).start()
            continue
        copy_of(u, k - 1).wait_recv()
        part, got = half >> k, lands[k - 1]
        if k < bits:
            acc[which, part : 2 * part, :, cols] += got[which, part : 2 * part, :, cols]
            copy_of(u, k).start()
            acc[which, 0:part, :, cols] += got[which, 0:part, :, cols]
            continue
        acc[which, 0:1, :, cols] += got[which, 0:1, :, cols]
        left[at, wide] -= 1
        if left[at, wide]:
            continue
        if not begun:
            small[3].wait()
            for g in range(groups):
                begin[g : g + 1, :] = accumulated[:, g * width : (g + 1) * width].astype(jnp.float32)
            begun = True
        running = begin[:, first:last]
        carried = jnp.zeros_like(running)
        for s in range(steps):
            adjusted = acc[s, 0, :, first:last] - carried
            new = (running + adjusted).astype(jnp.bfloat16).astype(jnp.float32)
            carried = (new - running) - adjusted
            running = new
            total = new - carried
            for t in range(wide):
                tops[s] = jnp.maximum(tops[s], jnp.abs(total[:, t * LANES : (t + 1) * LANES]))
            for g in range(groups):
                exact[s : s + 1, g * width + first : g * width + last] = total[g : g + 1, :]
        for g in range(groups):
            last_row[:, g * width + first : g * width + last] = total[g : g + 1, :]

    lane = lax.broadcasted_iota(jnp.int32, (1, LANES), 1)
    row = jnp.zeros((1, LANES), jnp.float32)
    for s in range(steps):
        top = jnp.max(jnp.max(tops[s], axis=0, keepdims=True), axis=1, keepdims=True)
        row = jnp.where(lane == s, top, row)
    peak[...] = row

    def everything(source, target, sent, received, device):
        return pltpu.make_async_remote_copy(
            src_ref=source,
            dst_ref=target,
            send_sem=sent,
            recv_sem=received,
            device_id={"dp": device},
            device_id_type=pl.DeviceIdType.MESH,
        )

    def peak_copy(j):
        return pltpu.make_async_remote_copy(
            src_ref=peak,
            dst_ref=table.at[me],
            send_sem=peak_send,
            recv_sem=peak_recv,
            device_id={"dp": me ^ (n - j)},
            device_id_type=pl.DeviceIdType.MESH,
        )

    def tell(j, carry):
        peak_copy(j).start()
        return carry

    lax.fori_loop(1, n, tell, 0)
    table[me] = row
    for k in range(bits):
        everything(lands[k], lands[k], send_sem.at[k], recv_sem.at[0], partners[0]).wait_send()
    others = everything(table.at[pl.ds(1, n - 1)], table.at[pl.ds(1, n - 1)], peak_send, peak_recv, partners[0])
    others.wait_send()
    others.wait_recv()
    buckets = exponents.shape[2]
    bucket_id = lax.broadcasted_iota(jnp.int32, (buckets, LANES), 0)
    lane_id = lax.broadcasted_iota(jnp.int32, (buckets, LANES), 1)
    by_bucket = jnp.zeros((buckets, LANES), jnp.float32)
    for i in range(n):
        by_bucket = jnp.maximum(by_bucket, jnp.where(bucket_id == bucket_of_row[i], table[i], 0.0))
    own = jnp.max(jnp.where(bucket_id == bucket_of_row[me], by_bucket, 0.0), axis=0, keepdims=True)
    for s in range(steps):
        turned = jnp.sum(jnp.where(bucket_id == lane_id, by_bucket[:, s : s + 1], 0.0), axis=0, keepdims=True)
        peak_table[s : s + 1, :] = turned[:, :buckets]
        scales[s : s + 1, :] = 1.0 / (jnp.broadcast_to(own[:, s : s + 1], (1, LANES)) + epsilon)


def finish(exact, last_row, peaks, scales, unit, peak_table, last, codes, sem):
    columns = exact.shape[1]
    copies = [
        pltpu.make_async_copy(last_row, last, sem.at[0]),
        pltpu.make_async_copy(peaks, peak_table, sem.at[1]),
    ]
    for copy in copies:
        copy.start()
    scale = scales[:, :1]
    half = columns // 2
    for h in range(2):
        part = pl.ds(h * half, half)
        codes[:, part] = (exact[:, part] * scale).astype(jnp.bfloat16)
        copies.append(pltpu.make_async_copy(codes.at[:, part], unit.at[:, part], sem.at[2 + h]))
        copies[-1].start()
    for copy in copies:
        copy.wait()


def on_device(n, tensor, grad_codes, exponents, accumulated, arrival, bucket_of_row):
    steps, _, rows, columns = grad_codes.shape
    buckets = exponents.shape[2]
    bits = n.bit_length() - 1
    groups = max(g for g in (1, 2, 4, 8) if columns % (g * LANES) == 0)
    width = columns // groups
    plan = plan_of(bits, width // LANES, steps)
    orders, units, _, cuts = plan
    half = rows // 2
    vmem = pl.BlockSpec(memory_space=pltpu.VMEM)
    operands = (grad_codes, exponents, accumulated, arrival, bucket_of_row)
    exact, last_row, peaks, scales = pl.pallas_call(
        functools.partial(exchange, n, plan),
        out_shape=(
            jax.ShapeDtypeStruct((steps, columns), jnp.float32),
            jax.ShapeDtypeStruct((1, columns), jnp.float32),
            jax.ShapeDtypeStruct((steps, buckets), jnp.float32),
            jax.ShapeDtypeStruct((steps, LANES), jnp.float32),
        ),
        in_specs=[pl.BlockSpec(memory_space=pltpu.HBM)] * 5,
        out_specs=(vmem,) * 4,
        scratch_shapes=[
            pltpu.SMEM(exponents.shape, jnp.int32),
            pltpu.VMEM(accumulated.shape, jnp.bfloat16),
            pltpu.SMEM(arrival.shape, jnp.int32),
            pltpu.SMEM(bucket_of_row.shape, jnp.int32),
            pltpu.SemaphoreType.DMA((4,)),
            pltpu.VMEM((steps, groups * rows, width), jnp.bfloat16),
            pltpu.VMEM((len(orders), steps, groups * rows, groups * rows), jnp.bfloat16),
            pltpu.VMEM((groups, width), jnp.float32),
            pltpu.VMEM((steps, half, groups, width), jnp.float32),
            pltpu.VMEM((steps, half, groups, width), jnp.float32),
            pltpu.VMEM((1, LANES), jnp.float32),
            pltpu.VMEM((n, 1, LANES), jnp.float32),
            pltpu.SemaphoreType.DMA((len(cuts) + 1,)),
            pltpu.SemaphoreType.DMA((bits,)),
            pltpu.SemaphoreType.DMA((max(slots_of(plan, bits).values()) + 1,)),
            pltpu.SemaphoreType.DMA,
            pltpu.SemaphoreType.DMA,
        ]
        + [pltpu.VMEM((steps, half >> k, groups, width), jnp.float32) for k in range(bits)],
        compiler_params=pltpu.CompilerParams(
            collective_id=0, has_side_effects=True, vmem_limit_bytes=VMEM_LIMIT
        ),
    )(*(pltpu.with_memory_space_constraint(a, pltpu.HBM) for a in operands))

    if tensor == 1:
        unit, peak_table, last = pl.pallas_call(
            finish,
            out_shape=(
                jax.ShapeDtypeStruct((steps, columns), jnp.bfloat16),
                jax.ShapeDtypeStruct((steps, buckets), jnp.float32),
                jax.ShapeDtypeStruct((1, columns), jnp.float32),
            ),
            in_specs=[vmem] * 4,
            out_specs=(pl.BlockSpec(memory_space=pltpu.HBM),) * 3,
            scratch_shapes=[pltpu.VMEM((steps, columns), jnp.bfloat16), pltpu.SemaphoreType.DMA((4,))],
            compiler_params=pltpu.CompilerParams(vmem_limit_bytes=8 * 1024 * 1024),
        )(exact, last_row, peaks, scales)
        return unit.reshape(steps, 1, columns), peak_table, last

    peak_table = lax.pmax(peaks, "tensor")
    own = lax.dynamic_slice_in_dim(bucket_of_row, lax.axis_index("dp"), 1, 0)
    own_member = own[:, None] == jnp.arange(buckets, dtype=jnp.int32)[None, :]
    own_peaks = jnp.max(jnp.where(own_member, peak_table, 0.0), axis=1, keepdims=True)
    unit = (exact / (own_peaks + epsilon)).astype(jnp.bfloat16)
    return unit.reshape(steps, 1, columns), peak_table, last_row


def solution(mesh):
    return jax.shard_map(
        functools.partial(on_device, mesh.shape["dp"], mesh.shape["tensor"]),
        mesh=mesh,
        in_specs=(P(None, "dp", None, "tensor"), P(None, "dp", None), P("dp", "tensor"), P(), P()),
        out_specs=(P(None, "dp", "tensor"), P(), P("dp", "tensor")),
        check_vma=False,
    )
```

```python
import functools

import jax
import jax.numpy as jnp
from jax import lax
from jax.experimental import pallas as pl
from jax.experimental.pallas import tpu as pltpu
from jax.sharding import PartitionSpec as P

epsilon = 1e-06
LANES = 128
VMEM_LIMIT = 48 * 1024 * 1024

ORDERS = [
    (0, 1, 2, 3, 4), (0, 2, 3, 1, 4), (0, 3, 1, 2, 4), (0, 2, 1, 3, 4),
    (0, 2, 3, 4, 1), (0, 1, 3, 4, 2), (0, 3, 1, 4, 2), (0, 3, 4, 1, 2),
    (0, 3, 4, 2, 1),
]
UNITS = [
    (0, 1, 0, 2, 7), (1, 1, 0, 2, 4), (1, 1, 2, 2, 5), (2, 1, 0, 2, 3), (3, 1, 0, 4, 3),
    (2, 1, 2, 2, 6), (4, 1, 0, 2, 5), (5, 1, 0, 4, 8), (6, 1, 0, 4, 0), (7, 1, 0, 4, 8),
    (8, 1, 0, 2, 2), (4, 1, 2, 2, 4), (9, 1, 0, 4, 1), (10, 1, 0, 4, 3), (11, 1, 0, 2, 1),
    (12, 1, 0, 4, 0), (13, 1, 0, 4, 0), (14, 1, 0, 4, 3), (8, 1, 2, 2, 1), (15, 1, 0, 4, 5),
    (16, 1, 0, 4, 0), (11, 1, 2, 2, 0), (17, 1, 0, 4, 3), (0, 1, 2, 2, 0),
]
TURNS = [
    0, 1, 2, 3, 4, 5, 0, 6, 1, 2, 7, 8, 5, 6, 3, 9, 4, 10, 7, 11, 12, 13, 14, 8,
    15, 9, 11, 16, 3, 17, 13, 18, 19, 16, 0, 2, 10, 18, 6, 14, 7, 20, 21, 5, 11, 8, 12, 17,
    1, 21, 22, 19, 18, 16, 5, 4, 13, 14, 22, 20, 9, 8, 3, 4, 6, 21, 15, 11, 13, 19, 3, 8,
    2, 1, 23, 17, 12, 13, 23, 14, 20, 16, 10, 3, 18, 15, 19, 22, 17, 21, 7, 1, 12, 4, 23, 14,
    20, 8, 16, 10, 0, 18, 15, 17, 22, 6, 5, 13, 23, 21, 12, 11, 9, 10, 19, 20, 15, 22, 5, 23,
    9, 6, 7, 11, 0, 14, 2, 21, 10, 18, 17, 19, 1, 16, 2, 0, 9, 20, 12, 22, 4, 15, 7, 23,
]
CUTS = (2, 6)


def plan_of(bits, tiles, steps):
    if bits == 5 and tiles == 18 and steps == 4:
        return ORDERS, UNITS, TURNS, CUTS
    head = list(range(1, min(4, bits)))
    tail = list(range(1 + len(head), bits))
    orders = [[0] + head[r:] + head[:r] + tail for r in range(max(1, len(head)))]
    units = [(t, 1, 0, steps, t % len(orders)) for t in range(tiles)]
    turns = [w - k for w in range(tiles + bits) for k in range(bits + 1) if 0 <= w - k < tiles]
    return orders, units, turns, (1,)


def slots_of(plan, bits):
    orders, units, turns, _ = plan
    seen, start, wait = [0] * len(units), {}, {}
    for at, u in enumerate(turns):
        k, seen[u] = seen[u], seen[u] + 1
        if k < bits:
            start[u, k] = at
        if k > 0:
            wait[u, k - 1] = at
    dim = {c: orders[units[c[0]][4]][c[1]] for c in start}
    slots, held = {}, []
    for c in sorted(start, key=start.get):
        there = [v for v in start if dim[v] == dim[c] and wait[v] <= start[c]]
        latest = max((start[v] for v in there), default=-1)
        for slot, last in enumerate(held):
            if wait[last] <= latest:
                slots[c], held[slot] = slot, c
                break
        else:
            slots[c] = len(held)
            held.append(c)
    return slots


def across(b):
    return (1 << b) | (b > 0)


def exchange(n, plan, codes, exponents_in, accumulated_in, arrival_in, bucket_in, exact, last_row, peak_table, scales, exponents,
             accumulated, arrival, bucket_of_row, small_sem, x, lhs, begin, out, acc, peak, table, x_sem, send_sem, recv_sem,
             peak_send, peak_recv, *lands):
    orders, units, turns, cuts = plan
    slots = slots_of(plan, n.bit_length() - 1)
    me = lax.axis_index("dp")
    bits = n.bit_length() - 1
    steps, size, width = x.shape
    rows = codes.shape[2]
    groups = size // rows
    half = rows // 2
    tiles = width // LANES

    small = [
        pltpu.make_async_copy(source, target, small_sem.at[k])
        for k, (source, target) in enumerate(
            [(arrival_in, arrival), (bucket_in, bucket_of_row), (exponents_in, exponents), (accumulated_in, accumulated)]
        )
    ]
    edges = [0, *(c for c in cuts if c < tiles), tiles]
    loads = []
    for c in range(len(edges) - 1):
        first, wide = edges[c] * LANES, (edges[c + 1] - edges[c]) * LANES
        loads.append(
            [
                pltpu.make_async_copy(
                    codes.at[:, 0, :, pl.ds(g * width + first, wide)],
                    x.at[:, pl.ds(g * rows, rows), pl.ds(first, wide)],
                    x_sem.at[c],
                )
                for g in range(groups)
            ]
        )
    for copy in small[:3] + loads[0]:
        copy.start()

    barrier = pltpu.get_barrier_semaphore()
    partners = []
    for b in range(bits):
        partners.append(me ^ across(b))
    for partner in partners:
        pl.semaphore_signal(barrier, inc=1, device_id={"dp": partner}, device_id_type=pl.DeviceIdType.MESH)
    for group in loads[1:]:
        for copy in group:
            copy.start()
    small[3].start()

    for copy in small[:3]:
        copy.wait()
    lane = lax.broadcasted_iota(jnp.int32, (1, size), 1)
    slot = lane & (rows - 1)
    held = jnp.zeros((1, size), jnp.int32)
    scale = [jnp.zeros((1, size), jnp.int32) for _ in range(steps)]
    for k in range(rows):
        row = arrival[k]
        bucket = bucket_of_row[row]
        here = slot == k
        held = jnp.where(here, row, held)
        for s in range(steps):
            scale[s] = jnp.where(here, exponents[s, 0, bucket], scale[s])
    scale = [jnp.exp2(-e.astype(jnp.float32)) for e in scale]
    row_shift = rows.bit_length() - 1
    group_shift = groups.bit_length() - 1
    wanted = ((held ^ me) << group_shift) + (lane >> row_shift)
    line = lax.broadcasted_iota(jnp.int32, (size, 1), 0)

    def spread(q, wanted_steps):
        target = line & (groups - 1)
        for m, b in enumerate(orders[q]):
            target = target ^ (((line >> (bits - 1 - m + group_shift)) & 1) * (across(b) << group_shift))
        mask = target == wanted
        for s in wanted_steps:
            lhs[q, s] = jnp.where(mask, scale[s], 0.0).astype(jnp.bfloat16)

    def copy_of(u, k):
        at, wide, s, count, q = units[u]
        cols, which, part = pl.ds(at * LANES, wide * LANES), pl.ds(s, count), half >> k
        source = out.at[which, :, :, cols] if k == 0 else acc.at[which, pl.ds(part, part), :, cols]
        return pltpu.make_async_remote_copy(
            src_ref=source,
            dst_ref=lands[k].at[which, :, :, cols],
            send_sem=send_sem.at[k],
            recv_sem=recv_sem.at[slots[u, k]],
            device_id={"dp": partners[orders[q][k]]},
            device_id_type=pl.DeviceIdType.MESH,
        )

    built, loaded, greeted = set(), 0, False
    done = [0] * len(units)
    left = {}
    for at, wide, *_ in units:
        left[at, wide] = left.get((at, wide), 0) + 1
    tops = [jnp.zeros((groups, LANES), jnp.float32) for _ in range(steps)]
    begun = False
    for u in turns:
        at, wide, s0, count, q = units[u]
        k, done[u] = done[u], done[u] + 1
        first, last, cols = at * LANES, (at + wide) * LANES, pl.ds(at * LANES, wide * LANES)
        which = pl.ds(s0, count)
        if k == 0:
            missing = [s for s in range(s0, s0 + count) if (q, s) not in built]
            if missing:
                spread(q, missing)
                built.update((q, s) for s in missing)
            while edges[loaded] < at + wide:
                chunk = x.at[:, :, pl.ds(edges[loaded] * LANES, (edges[loaded + 1] - edges[loaded]) * LANES)]
                pltpu.make_async_copy(chunk, chunk, x_sem.at[loaded]).wait()
                loaded += 1
            split = half * groups
            for s in range(s0, s0 + count):
                product = jnp.dot(lhs[q, s], x[s, :, cols], preferred_element_type=jnp.float32)
                out[s, :, :, cols] = product[split:].reshape(half, groups, last - first)
                acc[s, :, :, cols] = product[:split].reshape(half, groups, last - first)
            if not greeted:
                pl.semaphore_wait(barrier, bits)
                greeted = True
            copy_of(u, 0).start()
            continue
        copy_of(u, k - 1).wait_recv()
        part, got = half >> k, lands[k - 1]
        if k < bits:
            acc[which, part : 2 * part, :, cols] += got[which, part : 2 * part, :, cols]
            copy_of(u, k).start()
            acc[which, 0:part, :, cols] += got[which, 0:part, :, cols]
            continue
        acc[which, 0:1, :, cols] += got[which, 0:1, :, cols]
        left[at, wide] -= 1
        if left[at, wide]:
            continue
        if not begun:
            small[3].wait()
            for g in range(groups):
                begin[g : g + 1, :] = accumulated[:, g * width : (g + 1) * width].astype(jnp.float32)
            begun = True
        running = begin[:, first:last]
        carried = jnp.zeros_like(running)
        for s in range(steps):
            adjusted = acc[s, 0, :, first:last] - carried
            new = (running + adjusted).astype(jnp.bfloat16).astype(jnp.float32)
            carried = (new - running) - adjusted
            running = new
            total = new - carried
            for t in range(wide):
                tops[s] = jnp.maximum(tops[s], jnp.abs(total[:, t * LANES : (t + 1) * LANES]))
            for g in range(groups):
                exact[s : s + 1, g * width + first : g * width + last] = total[g : g + 1, :]
        for g in range(groups):
            last_row[:, g * width + first : g * width + last] = total[g : g + 1, :]

    lane = lax.broadcasted_iota(jnp.int32, (1, LANES), 1)
    row = jnp.zeros((1, LANES), jnp.float32)
    for s in range(steps):
        top = jnp.max(jnp.max(tops[s], axis=0, keepdims=True), axis=1, keepdims=True)
        row = jnp.where(lane == s, top, row)
    peak[...] = row

    def everything(source, target, sent, received, device):
        return pltpu.make_async_remote_copy(
            src_ref=source,
            dst_ref=target,
            send_sem=sent,
            recv_sem=received,
            device_id={"dp": device},
            device_id_type=pl.DeviceIdType.MESH,
        )

    def peak_copy(j):
        return pltpu.make_async_remote_copy(
            src_ref=peak,
            dst_ref=table.at[me],
            send_sem=peak_send,
            recv_sem=peak_recv,
            device_id={"dp": me ^ (n - j)},
            device_id_type=pl.DeviceIdType.MESH,
        )

    def tell(j, carry):
        peak_copy(j).start()
        return carry

    lax.fori_loop(1, n, tell, 0)
    table[me] = row
    for k in range(bits):
        everything(lands[k], lands[k], send_sem.at[k], recv_sem.at[0], partners[0]).wait_send()
    others = everything(table.at[pl.ds(1, n - 1)], table.at[pl.ds(1, n - 1)], peak_send, peak_recv, partners[0])
    others.wait_send()
    others.wait_recv()
    buckets = exponents.shape[2]
    bucket_id = lax.broadcasted_iota(jnp.int32, (buckets, LANES), 0)
    lane_id = lax.broadcasted_iota(jnp.int32, (buckets, LANES), 1)
    by_bucket = jnp.zeros((buckets, LANES), jnp.float32)
    for i in range(n):
        by_bucket = jnp.maximum(by_bucket, jnp.where(bucket_id == bucket_of_row[i], table[i], 0.0))
    own = jnp.max(jnp.where(bucket_id == bucket_of_row[me], by_bucket, 0.0), axis=0, keepdims=True)
    for s in range(steps):
        turned = jnp.sum(jnp.where(bucket_id == lane_id, by_bucket[:, s : s + 1], 0.0), axis=0, keepdims=True)
        peak_table[s : s + 1, :] = turned[:, :buckets]
        scales[s : s + 1, :] = 1.0 / (jnp.broadcast_to(own[:, s : s + 1], (1, LANES)) + epsilon)


def finish(exact, last_row, peaks, scales, unit, peak_table, last, codes, sem):
    columns = exact.shape[1]
    copies = [
        pltpu.make_async_copy(last_row, last, sem.at[0]),
        pltpu.make_async_copy(peaks, peak_table, sem.at[1]),
    ]
    for copy in copies:
        copy.start()
    scale = scales[:, :1]
    half = columns // 2
    for h in range(2):
        part = pl.ds(h * half, half)
        codes[:, part] = (exact[:, part] * scale).astype(jnp.bfloat16)
        copies.append(pltpu.make_async_copy(codes.at[:, part], unit.at[:, part], sem.at[2 + h]))
        copies[-1].start()
    for copy in copies:
        copy.wait()


def on_device(n, tensor, grad_codes, exponents, accumulated, arrival, bucket_of_row):
    steps, _, rows, columns = grad_codes.shape
    buckets = exponents.shape[2]
    bits = n.bit_length() - 1
    groups = max(g for g in (1, 2, 4, 8) if columns % (g * LANES) == 0)
    width = columns // groups
    plan = plan_of(bits, width // LANES, steps)
    orders, units, _, cuts = plan
    half = rows // 2
    vmem = pl.BlockSpec(memory_space=pltpu.VMEM)
    operands = (grad_codes, exponents, accumulated, arrival, bucket_of_row)
    exact, last_row, peaks, scales = pl.pallas_call(
        functools.partial(exchange, n, plan),
        out_shape=(
            jax.ShapeDtypeStruct((steps, columns), jnp.float32),
            jax.ShapeDtypeStruct((1, columns), jnp.float32),
            jax.ShapeDtypeStruct((steps, buckets), jnp.float32),
            jax.ShapeDtypeStruct((steps, LANES), jnp.float32),
        ),
        in_specs=[pl.BlockSpec(memory_space=pltpu.HBM)] * 5,
        out_specs=(vmem,) * 4,
        scratch_shapes=[
            pltpu.SMEM(exponents.shape, jnp.int32),
            pltpu.VMEM(accumulated.shape, jnp.bfloat16),
            pltpu.SMEM(arrival.shape, jnp.int32),
            pltpu.SMEM(bucket_of_row.shape, jnp.int32),
            pltpu.SemaphoreType.DMA((4,)),
            pltpu.VMEM((steps, groups * rows, width), jnp.bfloat16),
            pltpu.VMEM((len(orders), steps, groups * rows, groups * rows), jnp.bfloat16),
            pltpu.VMEM((groups, width), jnp.float32),
            pltpu.VMEM((steps, half, groups, width), jnp.float32),
            pltpu.VMEM((steps, half, groups, width), jnp.float32),
            pltpu.VMEM((1, LANES), jnp.float32),
            pltpu.VMEM((n, 1, LANES), jnp.float32),
            pltpu.SemaphoreType.DMA((len(cuts) + 1,)),
            pltpu.SemaphoreType.DMA((bits,)),
            pltpu.SemaphoreType.DMA((max(slots_of(plan, bits).values()) + 1,)),
            pltpu.SemaphoreType.DMA,
            pltpu.SemaphoreType.DMA,
        ]
        + [pltpu.VMEM((steps, half >> k, groups, width), jnp.float32) for k in range(bits)],
        compiler_params=pltpu.CompilerParams(
            collective_id=0, has_side_effects=True, vmem_limit_bytes=VMEM_LIMIT
        ),
    )(*(pltpu.with_memory_space_constraint(a, pltpu.HBM) for a in operands))

    if tensor == 1:
        unit, peak_table, last = pl.pallas_call(
            finish,
            out_shape=(
                jax.ShapeDtypeStruct((steps, columns), jnp.bfloat16),
                jax.ShapeDtypeStruct((steps, buckets), jnp.float32),
                jax.ShapeDtypeStruct((1, columns), jnp.float32),
            ),
            in_specs=[vmem] * 4,
            out_specs=(pl.BlockSpec(memory_space=pltpu.HBM),) * 3,
            scratch_shapes=[pltpu.VMEM((steps, columns), jnp.bfloat16), pltpu.SemaphoreType.DMA((4,))],
            compiler_params=pltpu.CompilerParams(vmem_limit_bytes=8 * 1024 * 1024),
        )(exact, last_row, peaks, scales)
        return unit.reshape(steps, 1, columns), peak_table, last

    peak_table = lax.pmax(peaks, "tensor")
    own = lax.dynamic_slice_in_dim(bucket_of_row, lax.axis_index("dp"), 1, 0)
    own_member = own[:, None] == jnp.arange(buckets, dtype=jnp.int32)[None, :]
    own_peaks = jnp.max(jnp.where(own_member, peak_table, 0.0), axis=1, keepdims=True)
    unit = (exact / (own_peaks + epsilon)).astype(jnp.bfloat16)
    return unit.reshape(steps, 1, columns), peak_table, last_row


def solution(mesh):
    return jax.shard_map(
        functools.partial(on_device, mesh.shape["dp"], mesh.shape["tensor"]),
        mesh=mesh,
        in_specs=(P(None, "dp", None, "tensor"), P(None, "dp", None), P("dp", "tensor"), P(), P()),
        out_specs=(P(None, "dp", "tensor"), P(), P("dp", "tensor")),
        check_vma=False,
    )
```
